1024 devices in a mesh: curve: 128 (over y, z), group: 8 (over x, core).
Axes of the slice: x: 4, y: 8, z: 16, core: 2. Of those that a mesh axis runs over, the one named last changes fastest.
Arguments:
- position: float32 [3, 16384, 128], P(None, ('curve', 'group')), may hold values from 0 to 2048
- mass: float32 [16384, 128], P(('curve', 'group')), may hold values from 0.003 to 0.03
- smooth: float32 [16384, 128], P(('curve', 'group')), may hold values from 0.25 to 1
- counts: int32 [16384], P(('curve', 'group')), may hold values from 8 to 128
- partners: int32 [16384, 8], P('curve'), may hold values from 0 to 16383, as said below
Outputs:
- density: float32 [16384, 128], P(('curve', 'group'))
- accel: float32 [3, 16384, 128], P(None, ('curve', 'group'))
The draws below stay inside these ranges and needn't reach their ends.
Inputs may be any that keep to these rules, and one draw needn't show every extreme that they name: partners[a, k] is a cell other than a whose distance to a along the cyclic curve order is 1 to 7; the 8 entries of a row differ.
All inputs are finite; a program needn't handle non-finite values.
Results may differ from the reference program's by a relative error of at most 0.0003.
Values sent between devices are 32-bit elements; how exact they have to be, the bound alone decides.
No kernel may reach another device: no remote copies, remote signals or barrier semaphores. Data moves between devices by JAX's collectives and lax.ppermute only.
A program may use at most 32 MiB of HBM per device.

```python
import math
import jax
import jax.numpy as jnp
from jax import lax

P_SIZE = 128
K = 8
REACH = 7
CELL_CURVE = 128
NCELL = 16384


def cell_grid(cells):
    halfway = NCELL // 2
    upper_lane = cells >= halfway
    mirrored = jnp.where(upper_lane, NCELL - 1 - cells, cells)
    layers = mirrored // 4
    within = mirrored % 4
    turned = jnp.where(layers % 2 == 0, within, 3 - within)
    across = jnp.where(turned >= 2, 1, 0).astype(jnp.int32)
    lateral = jnp.where((turned == 0) | (turned == 3), 1, 0).astype(jnp.int32)
    lateral = jnp.where(upper_lane, 3 - lateral, lateral).astype(jnp.int32)
    return (across, lateral, layers.astype(jnp.int32))


def cell_counts(key):
    groups_all = NCELL // CELL_CURVE
    levels = jax.random.randint(jax.random.fold_in(key, 31), (groups_all,), 0, 4)
    levels = levels.at[0].set(3)
    levels = levels.at[1].set(0)
    cells = jnp.arange(NCELL, dtype=jnp.int32)
    level_cell = levels[cells // CELL_CURVE]
    lowest = jnp.where(level_cell == 0, 8, jnp.where(level_cell == 1, 24, jnp.where(level_cell == 2, 56, 96)))
    highest = jnp.minimum(lowest + 48, P_SIZE + 1)
    drawn = jax.random.randint(jax.random.fold_in(key, 37), (NCELL,), lowest, highest)
    drawn = drawn.at[0].set(P_SIZE)
    drawn = drawn.at[CELL_CURVE].set(8)
    return drawn.astype(jnp.int32)


def draw_counts(key, part):
    return cell_counts(key)


def draw_partners(key, part):
    cells = jnp.arange(NCELL, dtype=jnp.int32)
    offsets = jnp.concatenate([jnp.arange(-REACH, 0, dtype=jnp.int32), jnp.arange(1, REACH + 1, dtype=jnp.int32)])
    candidate = (cells[:, None] + offsets[None, :]) % NCELL
    base_x, base_y, base_z = cell_grid(cells)
    cand_x, cand_y, cand_z = cell_grid(candidate)
    step_x = cand_x - base_x[:, None]
    step_y = cand_y - base_y[:, None]
    step_z = cand_z - base_z[:, None]
    spread = step_x * step_x + step_y * step_y + step_z * step_z
    noise = jax.random.randint(jax.random.fold_in(key, 17), (NCELL, 2 * REACH), 0, 12)
    scores = (spread * 4 + noise) * (2 * REACH) + jnp.arange(2 * REACH, dtype=jnp.int32)[None, :]
    order = jnp.argsort(scores, axis=1)[:, :K]
    return jnp.take_along_axis(candidate, order, axis=1).astype(jnp.int32)


def draw_position(key, part):
    cells = jnp.arange(NCELL, dtype=jnp.int32)
    across, lateral, layers = cell_grid(cells)
    centre = jnp.stack([across, lateral, layers], 0).astype(jnp.float32) + 0.5
    offset = jax.random.uniform(jax.random.fold_in(key, 41), (3, NCELL, P_SIZE), jnp.float32, -0.5, 0.5)
    return (centre[:, :, None] + offset).astype(jnp.float32)


def draw_smooth(key, part):
    live = cell_counts(key).astype(jnp.float32)
    spacing = jnp.exp(-jnp.log(live) / 3.0)
    factor = jnp.exp(jax.random.uniform(jax.random.fold_in(key, 43), (NCELL, P_SIZE), jnp.float32, jnp.log(0.8), jnp.log(1.25)))
    return jnp.clip(1.6 * spacing[:, None] * factor, 0.25, 1.0).astype(jnp.float32)


def shard_levels(stream_key, dims, shards, least, largest):
    def one(dim, shards_of):
        steps = jax.random.uniform(jax.random.fold_in(jax.random.fold_in(stream_key, 6), dim), (shards_of,), jnp.float32, least / len(shards), largest / len(shards))
        return jnp.repeat(jnp.exp(steps), dims[dim] // shards_of).reshape((-1,) + (1,) * (len(dims) - dim - 1))

    factor_of = one(*shards[0])
    for cut in shards[1:]:
        factor_of = factor_of * one(*cut)
    return factor_of


def setup_inputs(seed: int = 0) -> dict:
    streams_of = jax.random.split(jax.random.key(seed), 6)
    return {
        "position": draw_position(jax.random.fold_in(streams_of[5], 71), 0),
        "mass": jnp.clip(jnp.exp(math.log(0.03) - 2.3025851 * jax.random.uniform(streams_of[1], (NCELL, P_SIZE), jnp.float32) ** shard_levels(streams_of[1], (NCELL, P_SIZE), ((0, 1024),), -0.2, 0.2)), 0.003, 0.03),
        "smooth": draw_smooth(jax.random.fold_in(streams_of[5], 71), 0),
        "counts": draw_counts(jax.random.fold_in(streams_of[5], 71), 0),
        "partners": draw_partners(jax.random.fold_in(streams_of[5], 71), 0),
    }


def pair_sums(tpos, tsmooth, trecip, lists, table, force):
    count = lists.shape[0]
    width = lists.shape[1]
    slots = tpos.shape[-1]
    rows = table.shape[0]
    block = math.gcd(count, 4)
    blocks = count // block
    tp = tpos.reshape(3, blocks, block, slots).transpose(1, 0, 2, 3)
    tsb = tsmooth.reshape(blocks, block, slots)
    trb = trecip.reshape(blocks, block, slots)
    lsb = lists.reshape(blocks, block * width)

    def one(items):
        here, smooth_h, recip_h, listed = items
        source = jnp.take(table, listed, axis=1).reshape(rows, block, width * slots)
        delta = here[:, :, :, None] - source[:3, :, None, :]
        inv_sq = 1.0 / (smooth_h * smooth_h)
        weight = jnp.exp(-jnp.sum(delta * delta, 0) * inv_sq[..., None])
        if force:
            coeff = source[3][:, None, :] * (recip_h[..., None] + source[4][:, None, :]) * weight
            return 2.0 * inv_sq * jnp.sum(coeff * delta, -1)
        return jnp.sum(source[3][:, None, :] * weight, -1) * inv_sq / smooth_h

    result = lax.map(one, (tp, tsb, trb, lsb))
    if force:
        return result.transpose(1, 0, 2, 3).reshape(3, count, slots)
    return result.reshape(count, slots)


def reference(position, mass, smooth, counts, partners):
    slots = position.shape[-1]
    alive = jnp.arange(slots, dtype=jnp.int32)[None, :] < counts[:, None]
    mlive = jnp.where(alive, mass, jnp.zeros_like(mass))
    cells = jnp.arange(counts.shape[0], dtype=jnp.int32)[:, None]
    lists = jnp.concatenate([cells, partners.astype(jnp.int32)], 1)
    table = jnp.concatenate([position, mlive[None]], 0)
    zero = jnp.zeros_like(mass)
    density = pair_sums(position, smooth, zero, lists, table, False)
    density = jnp.where(alive, density, zero)
    recip = jnp.where(alive, 1.0 / jnp.where(alive, density, jnp.ones_like(density)), zero)
    table_f = jnp.concatenate([position, mlive[None], recip[None]], 0)
    accel = pair_sums(position, smooth, recip, lists, table_f, True)
    accel = jnp.where(alive[None], accel, jnp.zeros_like(accel))
    return density, accel
```

```python
import functools

import jax, jax.numpy as jnp
from jax import lax
from jax.experimental import pallas as pl
from jax.experimental.pallas import tpu as pltpu
from jax.sharding import PartitionSpec as P

LOG2E = 1.4426950408889634
HI = lax.Precision.HIGHEST
TABLE = 48
OWN = 16
CURVE = 128
NCELL = 16384
REACH = 7
KP = 8
X, Y, Z, M, H, S, R = range(7)


def body(odd_of, own, mate, peer, dens_ref, acc_ref, tab, bc, wts, part, row_f, ids, sems):
    odd = odd_of()
    sides = ((1, own), (2 - 2 * odd, mate), (2 * odd, peer))
    copies = []
    for n, (side, src) in enumerate(sides):
        copy = pltpu.make_async_copy(src.at[pl.ds(80, 8), :], ids.at[side], sems.at[n])
        copy.start()
        copies.append(copy)
    for side, src in sides:
        h = src[64:80, :]
        s = -LOG2E / (h * h)
        for p in range(16):
            for c in range(5):
                tab[side * 16 + p, c, :] = src[c * 16 + p, :]
            tab[side * 16 + p, S, :] = s[p]

    def columns(e, slot, chans):
        t = tab[e].T
        for n, c in chans:
            bc[slot, n] = jnp.broadcast_to(t[:, c : c + 1], (128, 128))

    def spread(i, _):
        columns(9 + i, i, ((0, X), (1, Y), (2, Z), (3, S)))
        return 0

    lax.fori_loop(0, 30, spread, 0, unroll=2)
    for copy in copies:
        copy.wait()

    def partner(e, k):
        side = e // 16
        return e + ids[side, k, e % 16].astype(jnp.int32)

    def bcast(e, c):
        return tab[e, pl.ds(c, 8, stride=0), :][None]

    def dens_cell(i, store):
        e = 9 + i
        who = [e] + [partner(e, k) for k in range(KP)]
        for g in range(4):
            rows = pl.ds(32 * g, 32)
            xi, yi, zi, si = [bc[i, n, rows, :].reshape(4, 8, 128) for n in range(4)]
            total = jnp.zeros((4, 8, 128), jnp.float32)
            for k, j in enumerate(who):
                dx = xi - bcast(j, X)
                dy = yi - bcast(j, Y)
                dz = zi - bcast(j, Z)
                w = jnp.exp2((dx * dx + dy * dy + dz * dz) * si) * bcast(j, M)
                total = total + w
                if store:
                    wts[i - 7, k, rows, :] = w.reshape(32, 128)
            part[i, rows, :] = total.reshape(32, 128)

    def own_dens(i, _):
        dens_cell(7 + i, True)
        return 0

    def rim_dens(i, _):
        dens_cell(jnp.where(i < 7, i, i + 16), False)
        return 0

    lax.fori_loop(0, 16, own_dens, 0)
    lax.fori_loop(0, 14, rim_dens, 0)
    ones = jnp.ones((8, 128), jnp.float32)

    def rowsum(v):
        return lax.dot_general(ones, v, (((1,), (1,)), ((), ())), precision=HI, preferred_element_type=jnp.float32)

    def finish(i, _):
        e = 9 + i
        t = rowsum(part[i])[0:1]
        h = tab[e, pl.ds(H, 1), :]
        live = tab[e, pl.ds(M, 1), :] > 0.0
        d = jnp.where(live, t / (h * h * h), 0.0)
        row_f[i] = jnp.broadcast_to(d, (8, 128))
        tab[e, pl.ds(R, 1), :] = jnp.where(live, 1.0 / jnp.where(live, d, 1.0), 0.0)
        return 0

    lax.fori_loop(0, 30, finish, 0, unroll=3)
    for p in range(16):
        dens_ref[p, :] = row_f[7 + p, 0]

    def spread_r(i, _):
        columns(16 + i, 7 + i, ((3, R),))
        return 0

    lax.fori_loop(0, 16, spread_r, 0, unroll=2)

    def force_cell(i, _):
        e = 16 + i
        who = [e] + [partner(e, k) for k in range(KP)]
        for g in range(4):
            rows = pl.ds(32 * g, 32)
            xi, yi, zi, ri = [bc[7 + i, n, rows, :].reshape(4, 8, 128) for n in range(4)]
            fx = fy = fz = jnp.zeros((4, 8, 128), jnp.float32)
            for k, j in enumerate(who):
                c = wts[i, k, rows, :].reshape(4, 8, 128) * (ri + bcast(j, R))
                fx = fx + c * (xi - bcast(j, X))
                fy = fy + c * (yi - bcast(j, Y))
                fz = fz + c * (zi - bcast(j, Z))
            bc[7 + i, 0, rows, :] = fx.reshape(32, 128)
            bc[7 + i, 1, rows, :] = fy.reshape(32, 128)
            bc[7 + i, 2, rows, :] = fz.reshape(32, 128)
        return 0

    lax.fori_loop(0, 16, force_cell, 0)

    def finish_f(i, _):
        e = 16 + i
        s = tab[e, pl.ds(S, 1), :]
        live = tab[e, pl.ds(M, 1), :] > 0.0
        scale = jnp.where(live, s * (-2.0 / LOG2E), 0.0)
        for n in range(3):
            row_f[i, n] = (rowsum(bc[7 + i, n])[0:1] * scale)[0]
        return 0

    lax.fori_loop(0, 16, finish_f, 0, unroll=2)
    for p in range(16):
        for n in range(3):
            acc_ref[n, p, :] = row_f[p, n]


def call(own, mate, peer, odd_of):
    f32 = jnp.float32
    return pl.pallas_call(
        functools.partial(body, odd_of),
        out_shape=(jax.ShapeDtypeStruct((16, 128), f32), jax.ShapeDtypeStruct((3, 16, 128), f32)),
        in_specs=[pl.BlockSpec(memory_space=pltpu.VMEM)] * 3,
        out_specs=(pl.BlockSpec(memory_space=pltpu.VMEM),) * 2,
        scratch_shapes=[
            pltpu.VMEM((TABLE, 8, 128), f32),
            pltpu.VMEM((30, 4, 128, 128), f32),
            pltpu.VMEM((16, 9, 128, 128), f32),
            pltpu.VMEM((30, 128, 128), f32),
            pltpu.VMEM((30, 8, 128), f32),
            pltpu.SMEM((3, 8, 128), f32),
            pltpu.SemaphoreType.DMA((3,)),
        ],
        compiler_params=pltpu.CompilerParams(vmem_limit_bytes=48 << 20),
        name="sph",
    )(own, mate, peer)


def shards(position, mass, smooth, counts, partners):
    groups = lax.axis_size("group")
    devices = groups * lax.axis_size("curve")
    group = lax.axis_index("group")
    start = lax.axis_index("curve") * CURVE
    slots = position.shape[-1]
    alive = jnp.arange(slots, dtype=jnp.int32)[None, :] < counts[:, None]
    mlive = jnp.where(alive, mass, jnp.zeros_like(mass))
    step = partners.T - (start + jnp.arange(CURVE, dtype=jnp.int32))[None, :]
    step = jnp.where(step > REACH, step - NCELL, jnp.where(step < -REACH, step + NCELL, step))
    step = lax.dynamic_slice_in_dim(step.astype(jnp.float32), group * OWN, OWN, 1)
    step = jnp.pad(step, ((0, 0), (0, slots - OWN)))
    packed = jnp.concatenate([position.reshape(3 * OWN, slots), mlive, smooth, step], 0)
    axes = ("curve", "group")
    chip = [(i, i ^ 1) for i in range(devices)]
    link = [(i, (i + 1 if i % 2 else i - 1) % devices) for i in range(devices)]
    over_link = lax.ppermute(packed, axes, link)
    over_chip = lax.ppermute(packed, axes, chip)
    return call(packed, over_chip, over_link, lambda: lax.rem(lax.axis_index("group"), 2))


def solution(mesh):
    return jax.shard_map(
        shards,
        mesh=mesh,
        in_specs=(
            P(None, ("curve", "group"), None),
            P(("curve", "group"), None),
            P(("curve", "group"), None),
            P(("curve", "group")),
            P("curve", None),
        ),
        out_specs=(P(("curve", "group"), None), P(None, ("curve", "group"), None)),
        check_vma=False,
    )
```

```python
import functools

import jax, jax.numpy as jnp
from jax import lax
from jax.experimental import pallas as pl
from jax.experimental.pallas import tpu as pltpu
from jax.sharding import PartitionSpec as P

LOG2E = 1.4426950408889634
HI = lax.Precision.HIGHEST
TABLE = 48
OWN = 16
CURVE = 128
NCELL = 16384
REACH = 7
KP = 8
X, Y, Z, M, H, S, R = range(7)
CM, CH, CS = 3, 4, 5


def partner(ids, e, k):
    return e + ids[e // 16, k, e % 16].astype(jnp.int32)


def direct(sides, dens_ref, acc_ref, tab, bc, wts, part, row_f, ids):
    for side, src in sides:
        h = src[64:80, :]
        s = -LOG2E / (h * h)
        for p in range(16):
            for c in range(5):
                tab[side * 16 + p, c, :] = src[c * 16 + p, :]
            tab[side * 16 + p, S, :] = s[p]

    def columns(e, slot, chans):
        t = tab[e].T
        for n, c in chans:
            bc[slot, n] = jnp.broadcast_to(t[:, c : c + 1], (128, 128))

    def spread(i, _):
        columns(9 + i, i, ((0, X), (1, Y), (2, Z), (3, S)))
        return 0

    lax.fori_loop(0, 30, spread, 0, unroll=2)
    def bcast(e, c):
        return tab[e, pl.ds(c, 8, stride=0), :][None]

    def dens_cell(i, store):
        e = 9 + i
        who = [e] + [partner(ids, e, k) for k in range(KP)]
        for g in range(4):
            rows = pl.ds(32 * g, 32)
            xi, yi, zi, si = [bc[i, n, rows, :].reshape(4, 8, 128) for n in range(4)]
            total = jnp.zeros((4, 8, 128), jnp.float32)
            for k, j in enumerate(who):
                dx = xi - bcast(j, X)
                dy = yi - bcast(j, Y)
                dz = zi - bcast(j, Z)
                w = jnp.exp2((dx * dx + dy * dy + dz * dz) * si) * bcast(j, M)
                total = total + w
                if store:
                    wts[i - 7, k, rows, :] = w.reshape(32, 128)
            part[i, rows, :] = total.reshape(32, 128)

    def own_dens(i, _):
        dens_cell(7 + i, True)
        return 0

    def rim_dens(i, _):
        dens_cell(jnp.where(i < 7, i, i + 16), False)
        return 0

    lax.fori_loop(0, 16, own_dens, 0)
    lax.fori_loop(0, 14, rim_dens, 0)
    ones = jnp.ones((8, 128), jnp.float32)

    def rowsum(v):
        return lax.dot_general(ones, v, (((1,), (1,)), ((), ())), precision=HI, preferred_element_type=jnp.float32)

    def finish(i, _):
        e = 9 + i
        t = rowsum(part[i])[0:1]
        h = tab[e, pl.ds(H, 1), :]
        live = tab[e, pl.ds(M, 1), :] > 0.0
        d = jnp.where(live, t / (h * h * h), 0.0)
        row_f[i] = jnp.broadcast_to(d, (8, 128))
        tab[e, pl.ds(R, 1), :] = jnp.where(live, 1.0 / jnp.where(live, d, 1.0), 0.0)
        return 0

    lax.fori_loop(0, 30, finish, 0, unroll=3)
    for p in range(16):
        dens_ref[p, :] = row_f[7 + p, 0]

    def spread_r(i, _):
        columns(16 + i, 7 + i, ((3, R),))
        return 0

    lax.fori_loop(0, 16, spread_r, 0, unroll=2)

    def force_cell(i, _):
        e = 16 + i
        who = [e] + [partner(ids, e, k) for k in range(KP)]
        for g in range(4):
            rows = pl.ds(32 * g, 32)
            xi, yi, zi, ri = [bc[7 + i, n, rows, :].reshape(4, 8, 128) for n in range(4)]
            fx = fy = fz = jnp.zeros((4, 8, 128), jnp.float32)
            for k, j in enumerate(who):
                c = wts[i, k, rows, :].reshape(4, 8, 128) * (ri + bcast(j, R))
                fx = fx + c * (xi - bcast(j, X))
                fy = fy + c * (yi - bcast(j, Y))
                fz = fz + c * (zi - bcast(j, Z))
            bc[7 + i, 0, rows, :] = fx.reshape(32, 128)
            bc[7 + i, 1, rows, :] = fy.reshape(32, 128)
            bc[7 + i, 2, rows, :] = fz.reshape(32, 128)
        return 0

    lax.fori_loop(0, 16, force_cell, 0)

    def finish_f(i, _):
        e = 16 + i
        s = tab[e, pl.ds(S, 1), :]
        live = tab[e, pl.ds(M, 1), :] > 0.0
        scale = jnp.where(live, s * (-2.0 / LOG2E), 0.0)
        for n in range(3):
            row_f[i, n] = (rowsum(bc[7 + i, n])[0:1] * scale)[0]
        return 0

    lax.fori_loop(0, 16, finish_f, 0, unroll=2)
    for p in range(16):
        for n in range(3):
            acc_ref[n, p, :] = row_f[p, n]


def split3(t):
    hi = t.astype(jnp.bfloat16).astype(jnp.float32)
    rest = t - hi
    mid = rest.astype(jnp.bfloat16).astype(jnp.float32)
    return hi, mid, (rest - mid).astype(jnp.bfloat16).astype(jnp.float32)


def expanded(dens_ref, acc_ref, com, tj, ti, left, right, rhs, whi, wlo, dsum, val, out, ids):
    bf16, f32 = jnp.bfloat16, jnp.float32
    lane = lax.broadcasted_iota(jnp.int32, (128, 128), 1)

    def columns(i, _):
        hi, mid, lo = split3(tj[2 + i])
        zero = jnp.zeros((8, 128), f32)
        half = [hi, mid, hi, lo, hi, mid, zero, zero]
        t = jnp.concatenate(half + half, 0).T
        left[2 + i] = jnp.where(lane < 64, t, 0.0).astype(bf16)
        right[2 + i] = jnp.where(lane < 64, 0.0, t).astype(bf16)
        return 0

    lax.fori_loop(0, 44, columns, 0, unroll=4)

    def rows(e):
        hi, mid, lo = split3(ti[e])
        zero = jnp.zeros((8, 128), f32)
        return jnp.concatenate([hi, hi, mid, hi, lo, mid, zero, zero], 0).astype(bf16)

    rim = [(0, 1), (2, 3), (4, 5), (6, 23), (24, 25), (26, 27), (28, 29)]
    blank = jnp.zeros((64, 128), bf16)
    for t, (i, j) in enumerate([(7 + 2 * t, 8 + 2 * t) for t in range(8)] + rim):
        rhs[t, 0:64, 0:128] = rows(9 + i)
        rhs[t, 0:64, 128:256] = blank
        rhs[t, 64:128, 0:128] = blank
        rhs[t, 64:128, 128:256] = rows(9 + j)

    def weights(t, i, j, store):
        a, b = 9 + i, 9 + j
        r = rhs[t]
        total = jnp.zeros((8, 256), f32)
        for k in range(KP + 1):
            p = a if k == 0 else partner(ids, a, k - 1)
            q = b if k == 0 else partner(ids, b, k - 1)
            e = jnp.dot(left[p] + right[q], r, preferred_element_type=f32)
            w = jnp.exp2(e)
            total = total + w.reshape(16, 8, 256).sum(0)
            if store:
                hi = w.astype(bf16)
                lo = (w - hi.astype(f32)).astype(bf16)
                at = pl.ds(128 * k, 128)
                whi[i - 7, at, :] = hi[:, :128]
                whi[j - 7, at, :] = hi[:, 128:]
                wlo[i - 7, at, :] = lo[:, :128]
                wlo[j - 7, at, :] = lo[:, 128:]
        dsum[i] = total[:, :128]
        dsum[j] = total[:, 128:]

    def own_pair(t, _):
        weights(t, 7 + 2 * t, 8 + 2 * t, True)
        return 0

    def rim_pair(t, _):
        i = jnp.where(t > 3, 16 + 2 * t, 2 * t)
        j = jnp.where(t > 2, 17 + 2 * t, 2 * t + 1)
        weights(8 + t, i, j, False)
        return 0

    lax.fori_loop(0, 8, own_pair, 0)
    lax.fori_loop(0, 7, rim_pair, 0)

    total = sum(dsum[:, n, :] for n in range(8))
    h = com[CH, 9:39, :]
    live = com[CM, 9:39, :] > 0.0
    dens = jnp.where(live, total / (h * h * h), 0.0)
    recip = jnp.where(live, 1.0 / jnp.where(live, dens, 1.0), 0.0)
    dens_ref[...] = dens[7:23]
    sub = lax.broadcasted_iota(jnp.int32, (8, 128), 0)
    zero = jnp.zeros((8, 128), f32)
    for i in range(30):
        t = tj[9 + i]
        v = jnp.where(sub < 4, t, pltpu.roll(t, 4, 0) * recip[i : i + 1])
        val[9 + i] = jnp.concatenate([*split3(v), zero], 0).astype(bf16)

    def force(i, _):
        e = 16 + i
        who = [e] + [partner(ids, e, k) for k in range(KP)]
        v = jnp.concatenate([val[j] for j in who], 1)
        o = jnp.dot(v, whi[i], preferred_element_type=f32) + jnp.dot(v, wlo[i], preferred_element_type=f32)
        out[i] = o[0:8] + o[8:16] + o[16:24]
        return 0

    lax.fori_loop(0, 16, force, 0, unroll=2)
    s = com[CS, 16:32, :]
    scale = jnp.where(live[7:23], s * (-2.0 / LOG2E), 0.0)
    r = recip[7:23]
    for n in range(3):
        u = com[n, 16:32, :]
        acc_ref[n] = scale * (r * (u * out[:, 0, :] - out[:, 1 + n, :]) + (u * out[:, 4, :] - out[:, 5 + n, :]))


def body(odd_of, own, mate, peer, dens_ref, acc_ref, com, tj, ti, left, right, rhs, whi, wlo, dsum, val, out,
         tab, bc, wts, part, row_f, ids, sems):
    odd = odd_of()
    sides = ((1, own), (2 - 2 * odd, mate), (2 * odd, peer))
    copies = []
    for n, (side, src) in enumerate(sides):
        copy = pltpu.make_async_copy(src.at[pl.ds(80, 8), :], ids.at[side], sems.at[n])
        copy.start()
        copies.append(copy)
    one = jnp.ones((1, 128), jnp.float32)
    centre = [jnp.broadcast_to(own[16 * c + 8 : 16 * c + 9, 0:1], (16, 128)) for c in range(3)]
    far = steep = jnp.zeros((16, 128), jnp.float32)
    for side, src in sides:
        u = [src[16 * c : 16 * c + 16, :] - centre[c] for c in range(3)]
        m = src[48:64, :]
        h = src[64:80, :]
        s = -LOG2E / (h * h)
        q = u[0] * u[0] + u[1] * u[1] + u[2] * u[2]
        lm = jnp.where(m > 0.0, jnp.log2(jnp.where(m > 0.0, m, 1.0)), -30000.0)
        far = jnp.maximum(far, q)
        steep = jnp.maximum(steep, -s)
        at = pl.ds(pl.multiple_of(side * 16, 16), 16)
        for c, x in enumerate((*u, m, h, s)):
            com[c, at, :] = x
        fi = (s * q, -2.0 * s * u[0], -2.0 * s * u[1], -2.0 * s * u[2], s)
        for p in range(16):
            e = side * 16 + p
            tj[e] = jnp.concatenate([one, *(x[p : p + 1] for x in (*u, q, lm)), 0.0 * one, 0.0 * one], 0)
            ti[e] = jnp.concatenate([*(x[p : p + 1] for x in fi), one, 0.0 * one, 0.0 * one], 0)
    near = jnp.max(far) * jnp.max(steep) < 2048.0
    for copy in copies:
        copy.wait()

    @pl.when(near)
    def _():
        expanded(dens_ref, acc_ref, com, tj, ti, left, right, rhs, whi, wlo, dsum, val, out, ids)

    @pl.when(jnp.logical_not(near))
    def _():
        direct(sides, dens_ref, acc_ref, tab, bc, wts, part, row_f, ids)


def call(own, mate, peer, odd_of):
    f32 = jnp.float32
    return pl.pallas_call(
        functools.partial(body, odd_of),
        out_shape=(jax.ShapeDtypeStruct((16, 128), f32), jax.ShapeDtypeStruct((3, 16, 128), f32)),
        in_specs=[pl.BlockSpec(memory_space=pltpu.VMEM)] * 3,
        out_specs=(pl.BlockSpec(memory_space=pltpu.VMEM),) * 2,
        scratch_shapes=[
            pltpu.VMEM((6, TABLE, 128), f32),
            pltpu.VMEM((TABLE, 8, 128), f32),
            pltpu.VMEM((TABLE, 8, 128), f32),
            pltpu.VMEM((TABLE, 128, 128), jnp.bfloat16),
            pltpu.VMEM((TABLE, 128, 128), jnp.bfloat16),
            pltpu.VMEM((15, 128, 256), jnp.bfloat16),
            pltpu.VMEM((16, 1152, 128), jnp.bfloat16),
            pltpu.VMEM((16, 1152, 128), jnp.bfloat16),
            pltpu.VMEM((30, 8, 128), f32),
            pltpu.VMEM((TABLE, 32, 128), jnp.bfloat16),
            pltpu.VMEM((16, 8, 128), f32),
            pltpu.VMEM((TABLE, 8, 128), f32),
            pltpu.VMEM((30, 4, 128, 128), f32),
            pltpu.VMEM((16, 9, 128, 128), f32),
            pltpu.VMEM((30, 128, 128), f32),
            pltpu.VMEM((30, 8, 128), f32),
            pltpu.SMEM((3, 8, 128), f32),
            pltpu.SemaphoreType.DMA((3,)),
        ],
        compiler_params=pltpu.CompilerParams(vmem_limit_bytes=56 << 20),
        name="sph",
    )(own, mate, peer)


def shards(position, mass, smooth, counts, partners):
    groups = lax.axis_size("group")
    devices = groups * lax.axis_size("curve")
    group = lax.axis_index("group")
    start = lax.axis_index("curve") * CURVE
    slots = position.shape[-1]
    alive = jnp.arange(slots, dtype=jnp.int32)[None, :] < counts[:, None]
    mlive = jnp.where(alive, mass, jnp.zeros_like(mass))
    step = partners.T - (start + jnp.arange(CURVE, dtype=jnp.int32))[None, :]
    step = jnp.where(step > REACH, step - NCELL, jnp.where(step < -REACH, step + NCELL, step))
    step = lax.dynamic_slice_in_dim(step.astype(jnp.float32), group * OWN, OWN, 1)
    step = jnp.pad(step, ((0, 0), (0, slots - OWN)))
    packed = jnp.concatenate([position.reshape(3 * OWN, slots), mlive, smooth, step], 0)
    axes = ("curve", "group")
    chip = [(i, i ^ 1) for i in range(devices)]
    link = [(i, (i + 1 if i % 2 else i - 1) % devices) for i in range(devices)]
    over_link = lax.ppermute(packed, axes, link)
    over_chip = lax.ppermute(packed, axes, chip)
    return call(packed, over_chip, over_link, lambda: lax.rem(lax.axis_index("group"), 2))


def solution(mesh):
    return jax.shard_map(
        shards,
        mesh=mesh,
        in_specs=(
            P(None, ("curve", "group"), None),
            P(("curve", "group"), None),
            P(("curve", "group"), None),
            P(("curve", "group")),
            P("curve", None),
        ),
        out_specs=(P(("curve", "group"), None), P(None, ("curve", "group"), None)),
        check_vma=False,
    )
```

```python
import functools

import jax, jax.numpy as jnp
from jax import lax
from jax.experimental import pallas as pl
from jax.experimental.pallas import tpu as pltpu
from jax.sharding import PartitionSpec as P


LOG2E = 1.4426950408889634
HI = lax.Precision.HIGHEST
TABLE = 48
OWN = 16
CURVE = 128
NCELL = 16384
REACH = 7
KP = 8
X, Y, Z, M, H, S, R = range(7)
CM, CH, CS = 3, 4, 5


def partner(ids, e, k):
    return e + ids[e // 16, k, e % 16].astype(jnp.int32)


def direct(sides, dens_ref, acc_ref, tab, bc, wts, part, row_f, ids):
    for side, src in sides:
        h = src[64:80, :]
        s = -LOG2E / (h * h)
        for p in range(16):
            for c in range(5):
                tab[side * 16 + p, c, :] = src[c * 16 + p, :]
            tab[side * 16 + p, S, :] = s[p]

    def columns(e, slot, chans):
        t = tab[e].T
        for n, c in chans:
            bc[slot, n] = jnp.broadcast_to(t[:, c : c + 1], (128, 128))

    def spread(i, _):
        columns(9 + i, i, ((0, X), (1, Y), (2, Z), (3, S)))
        return 0

    lax.fori_loop(0, 30, spread, 0, unroll=2)

    def bcast(e, c):
        return tab[e, pl.ds(c, 8, stride=0), :][None]

    def dens_cell(i, store):
        e = 9 + i
        who = [e] + [partner(ids, e, k) for k in range(KP)]
        for g in range(4):
            rows = pl.ds(32 * g, 32)
            xi, yi, zi, si = [bc[i, n, rows, :].reshape(4, 8, 128) for n in range(4)]
            total = jnp.zeros((4, 8, 128), jnp.float32)
            for k, j in enumerate(who):
                dx = xi - bcast(j, X)
                dy = yi - bcast(j, Y)
                dz = zi - bcast(j, Z)
                w = jnp.exp2((dx * dx + dy * dy + dz * dz) * si) * bcast(j, M)
                total = total + w
                if store:
                    wts[i - 7, k, rows, :] = w.reshape(32, 128)
            part[i, rows, :] = total.reshape(32, 128)

    def own_dens(i, _):
        dens_cell(7 + i, True)
        return 0

    def rim_dens(i, _):
        dens_cell(jnp.where(i < 7, i, i + 16), False)
        return 0

    lax.fori_loop(0, 16, own_dens, 0)
    lax.fori_loop(0, 14, rim_dens, 0)
    ones = jnp.ones((8, 128), jnp.float32)

    def rowsum(v):
        return lax.dot_general(ones, v, (((1,), (1,)), ((), ())), precision=HI, preferred_element_type=jnp.float32)

    def finish(i, _):
        e = 9 + i
        t = rowsum(part[i])[0:1]
        h = tab[e, pl.ds(H, 1), :]
        live = tab[e, pl.ds(M, 1), :] > 0.0
        d = jnp.where(live, t / (h * h * h), 0.0)
        row_f[i] = jnp.broadcast_to(d, (8, 128))
        tab[e, pl.ds(R, 1), :] = jnp.where(live, 1.0 / jnp.where(live, d, 1.0), 0.0)
        return 0

    lax.fori_loop(0, 30, finish, 0, unroll=3)
    for p in range(16):
        dens_ref[p, :] = row_f[7 + p, 0]

    def spread_r(i, _):
        columns(16 + i, 7 + i, ((3, R),))
        return 0

    lax.fori_loop(0, 16, spread_r, 0, unroll=2)

    def force_cell(i, _):
        e = 16 + i
        who = [e] + [partner(ids, e, k) for k in range(KP)]
        for g in range(4):
            rows = pl.ds(32 * g, 32)
            xi, yi, zi, ri = [bc[7 + i, n, rows, :].reshape(4, 8, 128) for n in range(4)]
            fx = fy = fz = jnp.zeros((4, 8, 128), jnp.float32)
            for k, j in enumerate(who):
                c = wts[i, k, rows, :].reshape(4, 8, 128) * (ri + bcast(j, R))
                fx = fx + c * (xi - bcast(j, X))
                fy = fy + c * (yi - bcast(j, Y))
                fz = fz + c * (zi - bcast(j, Z))
            bc[7 + i, 0, rows, :] = fx.reshape(32, 128)
            bc[7 + i, 1, rows, :] = fy.reshape(32, 128)
            bc[7 + i, 2, rows, :] = fz.reshape(32, 128)
        return 0

    lax.fori_loop(0, 16, force_cell, 0)

    def finish_f(i, _):
        e = 16 + i
        s = tab[e, pl.ds(S, 1), :]
        live = tab[e, pl.ds(M, 1), :] > 0.0
        scale = jnp.where(live, s * (-2.0 / LOG2E), 0.0)
        for n in range(3):
            row_f[i, n] = (rowsum(bc[7 + i, n])[0:1] * scale)[0]
        return 0

    lax.fori_loop(0, 16, finish_f, 0, unroll=2)
    for p in range(16):
        for n in range(3):
            acc_ref[n, p, :] = row_f[p, n]


def split3(t):
    hi = t.astype(jnp.bfloat16).astype(jnp.float32)
    rest = t - hi
    mid = rest.astype(jnp.bfloat16).astype(jnp.float32)
    return hi, mid, (rest - mid).astype(jnp.bfloat16).astype(jnp.float32)


def expanded(dens_ref, acc_ref, com, tj, ti, left, right, rhs, whi, wlo, dsum, val, out, ids):
    bf16, f32 = jnp.bfloat16, jnp.float32
    lane = lax.broadcasted_iota(jnp.int32, (128, 128), 1)

    def columns(i, _):
        hi, mid, lo = split3(tj[2 + i])
        zero = jnp.zeros((8, 128), f32)
        half = [hi, mid, hi, lo, hi, mid, zero, zero]
        t = jnp.concatenate(half + half, 0).T
        left[2 + i] = jnp.where(lane < 64, t, 0.0).astype(bf16)
        right[2 + i] = jnp.where(lane < 64, 0.0, t).astype(bf16)
        return 0

    lax.fori_loop(0, 44, columns, 0, unroll=11)

    def rows(e):
        hi, mid, lo = split3(ti[e])
        zero = jnp.zeros((8, 128), f32)
        return jnp.concatenate([hi, hi, mid, hi, lo, mid, zero, zero], 0).astype(bf16)

    rim = [(0, 1), (2, 3), (4, 5), (6, 23), (24, 25), (26, 27), (28, 29)]
    blank = jnp.zeros((64, 128), bf16)
    for t, (i, j) in enumerate([(7 + 2 * t, 8 + 2 * t) for t in range(8)] + rim):
        rhs[t, 0:64, 0:128] = rows(9 + i)
        rhs[t, 0:64, 128:256] = blank
        rhs[t, 64:128, 0:128] = blank
        rhs[t, 64:128, 128:256] = rows(9 + j)

    def weights(t, i, j, store):
        a, b = 9 + i, 9 + j
        r = rhs[t]
        total = jnp.zeros((8, 256), f32)
        for k in range(KP + 1):
            p = a if k == 0 else partner(ids, a, k - 1)
            q = b if k == 0 else partner(ids, b, k - 1)
            e = jnp.dot(left[p] + right[q], r, preferred_element_type=f32)
            w = jnp.exp2(e)
            total = total + w.reshape(16, 8, 256).sum(0)
            if store:
                hi = w.astype(bf16)
                lo = (w - hi.astype(f32)).astype(bf16)
                at = pl.ds(128 * k, 128)
                whi[i - 7, at, :] = hi[:, :128]
                whi[j - 7, at, :] = hi[:, 128:]
                wlo[i - 7, at, :] = lo[:, :128]
                wlo[j - 7, at, :] = lo[:, 128:]
        dsum[i] = total[:, :128]
        dsum[j] = total[:, 128:]

    def own_pair(t, _):
        weights(t, 7 + 2 * t, 8 + 2 * t, True)
        return 0

    def rim_pair(t, _):
        i = jnp.where(t > 3, 16 + 2 * t, 2 * t)
        j = jnp.where(t > 2, 17 + 2 * t, 2 * t + 1)
        weights(8 + t, i, j, False)
        return 0

    lax.fori_loop(0, 8, own_pair, 0, unroll=8)
    lax.fori_loop(0, 7, rim_pair, 0, unroll=7)

    total = sum(dsum[:, n, :] for n in range(8))
    h = com[CH, 9:39, :]
    live = com[CM, 9:39, :] > 0.0
    dens = jnp.where(live, total / (h * h * h), 0.0)
    recip = jnp.where(live, 1.0 / jnp.where(live, dens, 1.0), 0.0)
    dens_ref[...] = dens[7:23]
    sub = lax.broadcasted_iota(jnp.int32, (8, 128), 0)
    zero = jnp.zeros((8, 128), f32)
    for i in range(30):
        t = tj[9 + i]
        v = jnp.where(sub < 4, t, pltpu.roll(t, 4, 0) * recip[i : i + 1])
        val[9 + i] = jnp.concatenate([*split3(v), zero], 0).astype(bf16)

    def force(i, _):
        e = 16 + i
        who = [e] + [partner(ids, e, k) for k in range(KP)]
        v = jnp.concatenate([val[j] for j in who], 1)
        o = jnp.dot(v, whi[i], preferred_element_type=f32) + jnp.dot(v, wlo[i], preferred_element_type=f32)
        out[i] = o[0:8] + o[8:16] + o[16:24]
        return 0

    lax.fori_loop(0, 16, force, 0, unroll=8)
    s = com[CS, 16:32, :]
    scale = jnp.where(live[7:23], s * (-2.0 / LOG2E), 0.0)
    r = recip[7:23]
    for n in range(3):
        u = com[n, 16:32, :]
        acc_ref[n] = scale * (r * (u * out[:, 0, :] - out[:, 1 + n, :]) + (u * out[:, 4, :] - out[:, 5 + n, :]))


def body(odd_of, own, mate, peer, dens_ref, acc_ref, com, tj, ti, left, right, rhs, whi, wlo, dsum, val, out,
         tab, bc, wts, part, row_f, ids, sems):
    odd = odd_of()
    sides = ((1, own), (2 - 2 * odd, mate), (2 * odd, peer))
    copies = []
    for n, (side, src) in enumerate(sides):
        copy = pltpu.make_async_copy(src.at[pl.ds(80, 8), :], ids.at[side], sems.at[n])
        copy.start()
        copies.append(copy)
    one = jnp.ones((1, 128), jnp.float32)
    centre = [jnp.broadcast_to(own[16 * c + 8 : 16 * c + 9, 0:1], (16, 128)) for c in range(3)]
    far = steep = jnp.zeros((16, 128), jnp.float32)
    for side, src in sides:
        u = [src[16 * c : 16 * c + 16, :] - centre[c] for c in range(3)]
        m = src[48:64, :]
        h = src[64:80, :]
        s = -LOG2E / (h * h)
        q = u[0] * u[0] + u[1] * u[1] + u[2] * u[2]
        lm = jnp.where(m > 0.0, jnp.log2(jnp.where(m > 0.0, m, 1.0)), -30000.0)
        far = jnp.maximum(far, q)
        steep = jnp.maximum(steep, -s)
        at = pl.ds(pl.multiple_of(side * 16, 16), 16)
        for c, x in enumerate((*u, m, h, s)):
            com[c, at, :] = x
        fi = (s * q, -2.0 * s * u[0], -2.0 * s * u[1], -2.0 * s * u[2], s)
        for p in range(16):
            e = side * 16 + p
            tj[e] = jnp.concatenate([one, *(x[p : p + 1] for x in (*u, q, lm)), 0.0 * one, 0.0 * one], 0)
            ti[e] = jnp.concatenate([*(x[p : p + 1] for x in fi), one, 0.0 * one, 0.0 * one], 0)
    near = jnp.max(far) * jnp.max(steep) < 2048.0
    for copy in copies:
        copy.wait()

    @pl.when(near)
    def _():
        expanded(dens_ref, acc_ref, com, tj, ti, left, right, rhs, whi, wlo, dsum, val, out, ids)

    @pl.when(jnp.logical_not(near))
    def _():
        direct(sides, dens_ref, acc_ref, tab, bc, wts, part, row_f, ids)


def call(own, mate, peer, odd_of):
    f32 = jnp.float32
    return pl.pallas_call(
        functools.partial(body, odd_of),
        out_shape=(jax.ShapeDtypeStruct((16, 128), f32), jax.ShapeDtypeStruct((3, 16, 128), f32)),
        in_specs=[pl.BlockSpec(memory_space=pltpu.VMEM)] * 3,
        out_specs=(pl.BlockSpec(memory_space=pltpu.VMEM),) * 2,
        scratch_shapes=[
            pltpu.VMEM((6, TABLE, 128), f32),
            pltpu.VMEM((TABLE, 8, 128), f32),
            pltpu.VMEM((TABLE, 8, 128), f32),
            pltpu.VMEM((TABLE, 128, 128), jnp.bfloat16),
            pltpu.VMEM((TABLE, 128, 128), jnp.bfloat16),
            pltpu.VMEM((15, 128, 256), jnp.bfloat16),
            pltpu.VMEM((16, 1152, 128), jnp.bfloat16),
            pltpu.VMEM((16, 1152, 128), jnp.bfloat16),
            pltpu.VMEM((30, 8, 128), f32),
            pltpu.VMEM((TABLE, 32, 128), jnp.bfloat16),
            pltpu.VMEM((16, 8, 128), f32),
            pltpu.VMEM((TABLE, 8, 128), f32),
            pltpu.VMEM((30, 4, 128, 128), f32),
            pltpu.VMEM((16, 9, 128, 128), f32),
            pltpu.VMEM((30, 128, 128), f32),
            pltpu.VMEM((30, 8, 128), f32),
            pltpu.SMEM((3, 8, 128), f32),
            pltpu.SemaphoreType.DMA((3,)),
        ],
        compiler_params=pltpu.CompilerParams(vmem_limit_bytes=40 << 20),
        name="sph",
    )(own, mate, peer)


def shards(position, mass, smooth, counts, partners):
    groups = lax.axis_size("group")
    devices = groups * lax.axis_size("curve")
    group = lax.axis_index("group")
    start = lax.axis_index("curve") * CURVE
    slots = position.shape[-1]
    alive = jnp.arange(slots, dtype=jnp.int32)[None, :] < counts[:, None]
    mlive = jnp.where(alive, mass, jnp.zeros_like(mass))
    step = partners.T - (start + jnp.arange(CURVE, dtype=jnp.int32))[None, :]
    step = jnp.where(step > REACH, step - NCELL, jnp.where(step < -REACH, step + NCELL, step))
    step = lax.dynamic_slice_in_dim(step.astype(jnp.float32), group * OWN, OWN, 1)
    step = jnp.pad(step, ((0, 0), (0, slots - OWN)))
    packed = jnp.concatenate([position.reshape(3 * OWN, slots), mlive, smooth, step], 0)
    axes = ("curve", "group")
    chip = [(i, i ^ 1) for i in range(devices)]
    link = [(i, (i + 1 if i % 2 else i - 1) % devices) for i in range(devices)]
    over_chip = lax.ppermute(packed, axes, chip)
    over_link = lax.ppermute(packed, axes, link)
    return call(packed, over_chip, over_link, lambda: lax.rem(lax.axis_index("group"), 2))


def solution(mesh):
    return jax.shard_map(
        shards,
        mesh=mesh,
        in_specs=(
            P(None, ("curve", "group"), None),
            P(("curve", "group"), None),
            P(("curve", "group"), None),
            P(("curve", "group")),
            P("curve", None),
        ),
        out_specs=(P(("curve", "group"), None), P(None, ("curve", "group"), None)),
        check_vma=False,
    )
```

```python
import functools

import jax, jax.numpy as jnp
from jax import lax
from jax.experimental import pallas as pl
from jax.experimental.pallas import tpu as pltpu
from jax.sharding import PartitionSpec as P


LOG2E = 1.4426950408889634
HI = lax.Precision.HIGHEST
TABLE = 48
OWN = 16
CURVE = 128
NCELL = 16384
REACH = 7
KP = 8
X, Y, Z, M, H, S, R = range(7)
CM, CH, CS = 3, 4, 5


def partner(ids, e, k):
    return e + ids[e // 16, k, e % 16].astype(jnp.int32)


def direct(sides, dens_ref, acc_ref, tab, bc, wts, part, row_f, ids):
    for side, src in sides:
        h = src[64:80, :]
        s = -LOG2E / (h * h)
        for p in range(16):
            for c in range(5):
                tab[side * 16 + p, c, :] = src[c * 16 + p, :]
            tab[side * 16 + p, S, :] = s[p]

    def columns(e, slot, chans):
        t = tab[e].T
        for n, c in chans:
            bc[slot, n] = jnp.broadcast_to(t[:, c : c + 1], (128, 128))

    def spread(i, _):
        columns(9 + i, i, ((0, X), (1, Y), (2, Z), (3, S)))
        return 0

    lax.fori_loop(0, 30, spread, 0, unroll=2)

    def bcast(e, c):
        return tab[e, pl.ds(c, 8, stride=0), :][None]

    def dens_cell(i, store):
        e = 9 + i
        who = [e] + [partner(ids, e, k) for k in range(KP)]
        for g in range(4):
            rows = pl.ds(32 * g, 32)
            xi, yi, zi, si = [bc[i, n, rows, :].reshape(4, 8, 128) for n in range(4)]
            total = jnp.zeros((4, 8, 128), jnp.float32)
            for k, j in enumerate(who):
                dx = xi - bcast(j, X)
                dy = yi - bcast(j, Y)
                dz = zi - bcast(j, Z)
                w = jnp.exp2((dx * dx + dy * dy + dz * dz) * si) * bcast(j, M)
                total = total + w
                if store:
                    wts[i - 7, k, rows, :] = w.reshape(32, 128)
            part[i, rows, :] = total.reshape(32, 128)

    def own_dens(i, _):
        dens_cell(7 + i, True)
        return 0

    def rim_dens(i, _):
        dens_cell(jnp.where(i < 7, i, i + 16), False)
        return 0

    lax.fori_loop(0, 16, own_dens, 0)
    lax.fori_loop(0, 14, rim_dens, 0)
    ones = jnp.ones((8, 128), jnp.float32)

    def rowsum(v):
        return lax.dot_general(ones, v, (((1,), (1,)), ((), ())), precision=HI, preferred_element_type=jnp.float32)

    def finish(i, _):
        e = 9 + i
        t = rowsum(part[i])[0:1]
        h = tab[e, pl.ds(H, 1), :]
        live = tab[e, pl.ds(M, 1), :] > 0.0
        d = jnp.where(live, t / (h * h * h), 0.0)
        row_f[i] = jnp.broadcast_to(d, (8, 128))
        tab[e, pl.ds(R, 1), :] = jnp.where(live, 1.0 / jnp.where(live, d, 1.0), 0.0)
        return 0

    lax.fori_loop(0, 30, finish, 0, unroll=3)
    for p in range(16):
        dens_ref[p, :] = row_f[7 + p, 0]

    def spread_r(i, _):
        columns(16 + i, 7 + i, ((3, R),))
        return 0

    lax.fori_loop(0, 16, spread_r, 0, unroll=2)

    def force_cell(i, _):
        e = 16 + i
        who = [e] + [partner(ids, e, k) for k in range(KP)]
        for g in range(4):
            rows = pl.ds(32 * g, 32)
            xi, yi, zi, ri = [bc[7 + i, n, rows, :].reshape(4, 8, 128) for n in range(4)]
            fx = fy = fz = jnp.zeros((4, 8, 128), jnp.float32)
            for k, j in enumerate(who):
                c = wts[i, k, rows, :].reshape(4, 8, 128) * (ri + bcast(j, R))
                fx = fx + c * (xi - bcast(j, X))
                fy = fy + c * (yi - bcast(j, Y))
                fz = fz + c * (zi - bcast(j, Z))
            bc[7 + i, 0, rows, :] = fx.reshape(32, 128)
            bc[7 + i, 1, rows, :] = fy.reshape(32, 128)
            bc[7 + i, 2, rows, :] = fz.reshape(32, 128)
        return 0

    lax.fori_loop(0, 16, force_cell, 0)

    def finish_f(i, _):
        e = 16 + i
        s = tab[e, pl.ds(S, 1), :]
        live = tab[e, pl.ds(M, 1), :] > 0.0
        scale = jnp.where(live, s * (-2.0 / LOG2E), 0.0)
        for n in range(3):
            row_f[i, n] = (rowsum(bc[7 + i, n])[0:1] * scale)[0]
        return 0

    lax.fori_loop(0, 16, finish_f, 0, unroll=2)
    for p in range(16):
        for n in range(3):
            acc_ref[n, p, :] = row_f[p, n]


def split3(t):
    hi = t.astype(jnp.bfloat16).astype(jnp.float32)
    rest = t - hi
    mid = rest.astype(jnp.bfloat16).astype(jnp.float32)
    return hi, mid, (rest - mid).astype(jnp.bfloat16).astype(jnp.float32)


def expanded(dens_ref, acc_ref, com, tj, ti, left, right, rhs, whi, wlo, dsum, val, out, ids):
    bf16, f32 = jnp.bfloat16, jnp.float32
    lane = lax.broadcasted_iota(jnp.int32, (128, 128), 1)

    def columns(i, _):
        hi, mid, lo = split3(tj[2 + i])
        zero = jnp.zeros((8, 128), f32)
        half = [hi, mid, hi, lo, hi, mid, zero, zero]
        t = jnp.concatenate(half + half, 0).T
        left[2 + i] = jnp.where(lane < 64, t, 0.0).astype(bf16)
        right[2 + i] = jnp.where(lane < 64, 0.0, t).astype(bf16)
        return 0

    lax.fori_loop(0, 44, columns, 0, unroll=22)

    def rows(e):
        hi, mid, lo = split3(ti[e])
        zero = jnp.zeros((8, 128), f32)
        return jnp.concatenate([hi, hi, mid, hi, lo, mid, zero, zero], 0).astype(bf16)

    rim = [(0, 1), (2, 3), (4, 5), (6, 23), (24, 25), (26, 27), (28, 29)]
    blank = jnp.zeros((64, 128), bf16)
    for t, (i, j) in enumerate([(7 + 2 * t, 8 + 2 * t) for t in range(8)] + rim):
        rhs[t, 0:64, 0:128] = rows(9 + i)
        rhs[t, 0:64, 128:256] = blank
        rhs[t, 64:128, 0:128] = blank
        rhs[t, 64:128, 128:256] = rows(9 + j)

    def weights(t, i, j, store):
        a, b = 9 + i, 9 + j
        r = rhs[t]
        total = jnp.zeros((8, 256), f32)
        for k in range(KP + 1):
            p = a if k == 0 else partner(ids, a, k - 1)
            q = b if k == 0 else partner(ids, b, k - 1)
            e = jnp.dot(left[p] + right[q], r, preferred_element_type=f32)
            w = jnp.exp2(e)
            total = total + w.reshape(16, 8, 256).sum(0)
            if store:
                hi = w.astype(bf16)
                lo = (w - hi.astype(f32)).astype(bf16)
                at = pl.ds(128 * k, 128)
                whi[i - 7, at, :] = hi[:, :128]
                whi[j - 7, at, :] = hi[:, 128:]
                wlo[i - 7, at, :] = lo[:, :128]
                wlo[j - 7, at, :] = lo[:, 128:]
        dsum[i] = total[:, :128]
        dsum[j] = total[:, 128:]

    def own_pair(t, _):
        weights(t, 7 + 2 * t, 8 + 2 * t, True)
        return 0

    def rim_pair(t, _):
        i = jnp.where(t > 3, 16 + 2 * t, 2 * t)
        j = jnp.where(t > 2, 17 + 2 * t, 2 * t + 1)
        weights(8 + t, i, j, False)
        return 0

    lax.fori_loop(0, 8, own_pair, 0, unroll=8)
    lax.fori_loop(0, 7, rim_pair, 0, unroll=7)

    total = sum(dsum[:, n, :] for n in range(8))
    h = com[CH, 9:39, :]
    live = com[CM, 9:39, :] > 0.0
    dens = jnp.where(live, total / (h * h * h), 0.0)
    recip = jnp.where(live, 1.0 / jnp.where(live, dens, 1.0), 0.0)
    dens_ref[...] = dens[7:23]
    sub = lax.broadcasted_iota(jnp.int32, (8, 128), 0)
    zero = jnp.zeros((8, 128), f32)
    for i in range(30):
        t = tj[9 + i]
        v = jnp.where(sub < 4, t, pltpu.roll(t, 4, 0) * recip[i : i + 1])
        val[9 + i] = jnp.concatenate([*split3(v), zero], 0).astype(bf16)

    def force(i, _):
        e = 16 + i
        who = [e] + [partner(ids, e, k) for k in range(KP)]
        v = jnp.concatenate([val[j] for j in who], 1)
        o = jnp.dot(v, whi[i], preferred_element_type=f32) + jnp.dot(v, wlo[i], preferred_element_type=f32)
        out[i] = o[0:8] + o[8:16] + o[16:24]
        return 0

    lax.fori_loop(0, 16, force, 0, unroll=16)
    s = com[CS, 16:32, :]
    scale = jnp.where(live[7:23], s * (-2.0 / LOG2E), 0.0)
    r = recip[7:23]
    for n in range(3):
        u = com[n, 16:32, :]
        acc_ref[n] = scale * (r * (u * out[:, 0, :] - out[:, 1 + n, :]) + (u * out[:, 4, :] - out[:, 5 + n, :]))


def body(odd_of, own, mate, peer, dens_ref, acc_ref, com, tj, ti, left, right, rhs, whi, wlo, dsum, val, out,
         tab, bc, wts, part, row_f, ids, sems):
    odd = odd_of()
    sides = ((1, own), (2 - 2 * odd, mate), (2 * odd, peer))
    copies = []
    for n, (side, src) in enumerate(sides):
        copy = pltpu.make_async_copy(src.at[pl.ds(80, 8), :], ids.at[side], sems.at[n])
        copy.start()
        copies.append(copy)
    one = jnp.ones((1, 128), jnp.float32)
    centre = [jnp.broadcast_to(own[16 * c + 8 : 16 * c + 9, 0:1], (16, 128)) for c in range(3)]
    far = steep = jnp.zeros((16, 128), jnp.float32)
    for side, src in sides:
        u = [src[16 * c : 16 * c + 16, :] - centre[c] for c in range(3)]
        m = src[48:64, :]
        h = src[64:80, :]
        s = -LOG2E / (h * h)
        q = u[0] * u[0] + u[1] * u[1] + u[2] * u[2]
        lm = jnp.where(m > 0.0, jnp.log2(jnp.where(m > 0.0, m, 1.0)), -30000.0)
        far = jnp.maximum(far, q)
        steep = jnp.maximum(steep, -s)
        at = pl.ds(pl.multiple_of(side * 16, 16), 16)
        for c, x in enumerate((*u, m, h, s)):
            com[c, at, :] = x
        fi = (s * q, -2.0 * s * u[0], -2.0 * s * u[1], -2.0 * s * u[2], s)
        for p in range(16):
            e = side * 16 + p
            tj[e] = jnp.concatenate([one, *(x[p : p + 1] for x in (*u, q, lm)), 0.0 * one, 0.0 * one], 0)
            ti[e] = jnp.concatenate([*(x[p : p + 1] for x in fi), one, 0.0 * one, 0.0 * one], 0)
    near = jnp.max(far) * jnp.max(steep) < 2048.0
    for copy in copies:
        copy.wait()

    @pl.when(near)
    def _():
        expanded(dens_ref, acc_ref, com, tj, ti, left, right, rhs, whi, wlo, dsum, val, out, ids)

    @pl.when(jnp.logical_not(near))
    def _():
        direct(sides, dens_ref, acc_ref, tab, bc, wts, part, row_f, ids)


def call(own, mate, peer, odd_of):
    f32 = jnp.float32
    return pl.pallas_call(
        functools.partial(body, odd_of),
        out_shape=(jax.ShapeDtypeStruct((16, 128), f32), jax.ShapeDtypeStruct((3, 16, 128), f32)),
        in_specs=[pl.BlockSpec(memory_space=pltpu.VMEM)] * 3,
        out_specs=(pl.BlockSpec(memory_space=pltpu.VMEM),) * 2,
        scratch_shapes=[
            pltpu.VMEM((6, TABLE, 128), f32),
            pltpu.VMEM((TABLE, 8, 128), f32),
            pltpu.VMEM((TABLE, 8, 128), f32),
            pltpu.VMEM((TABLE, 128, 128), jnp.bfloat16),
            pltpu.VMEM((TABLE, 128, 128), jnp.bfloat16),
            pltpu.VMEM((15, 128, 256), jnp.bfloat16),
            pltpu.VMEM((16, 1152, 128), jnp.bfloat16),
            pltpu.VMEM((16, 1152, 128), jnp.bfloat16),
            pltpu.VMEM((30, 8, 128), f32),
            pltpu.VMEM((TABLE, 32, 128), jnp.bfloat16),
            pltpu.VMEM((16, 8, 128), f32),
            pltpu.VMEM((TABLE, 8, 128), f32),
            pltpu.VMEM((30, 4, 128, 128), f32),
            pltpu.VMEM((16, 9, 128, 128), f32),
            pltpu.VMEM((30, 128, 128), f32),
            pltpu.VMEM((30, 8, 128), f32),
            pltpu.SMEM((3, 8, 128), f32),
            pltpu.SemaphoreType.DMA((3,)),
        ],
        compiler_params=pltpu.CompilerParams(vmem_limit_bytes=40 << 20),
        name="sph",
    )(own, mate, peer)


def shards(position, mass, smooth, counts, partners):
    groups = lax.axis_size("group")
    devices = groups * lax.axis_size("curve")
    group = lax.axis_index("group")
    start = lax.axis_index("curve") * CURVE
    slots = position.shape[-1]
    alive = jnp.arange(slots, dtype=jnp.int32)[None, :] < counts[:, None]
    mlive = jnp.where(alive, mass, jnp.zeros_like(mass))
    step = partners.T - (start + jnp.arange(CURVE, dtype=jnp.int32))[None, :]
    step = jnp.where(step > REACH, step - NCELL, jnp.where(step < -REACH, step + NCELL, step))
    step = lax.dynamic_slice_in_dim(step.astype(jnp.float32), group * OWN, OWN, 1)
    step = jnp.pad(step, ((0, 0), (0, slots - OWN)))
    packed = jnp.concatenate([position.reshape(3 * OWN, slots), mlive, smooth, step], 0)
    axes = ("curve", "group")
    edge = [(0, 1), (1, 0)]
    chip = [(i, i ^ 1) for i in range(2, devices)]
    link = [(i, (i + 1 if i % 2 else i - 1) % devices) for i in range(devices)]
    first = lax.ppermute(packed, axes, edge)
    over_link = lax.ppermute(packed, axes, link)
    over_chip = first + lax.ppermute(packed, axes, chip)
    return call(packed, over_chip, over_link, lambda: lax.rem(lax.axis_index("group"), 2))


def solution(mesh):
    return jax.shard_map(
        shards,
        mesh=mesh,
        in_specs=(
            P(None, ("curve", "group"), None),
            P(("curve", "group"), None),
            P(("curve", "group"), None),
            P(("curve", "group")),
            P("curve", None),
        ),
        out_specs=(P(("curve", "group"), None), P(None, ("curve", "group"), None)),
        check_vma=False,
    )
```

```python
import functools

import jax, jax.numpy as jnp
from jax import lax
from jax.experimental import pallas as pl
from jax.experimental.pallas import tpu as pltpu
from jax.sharding import PartitionSpec as P


LOG2E = 1.4426950408889634
HI = lax.Precision.HIGHEST
TABLE = 48
OWN = 16
CURVE = 128
NCELL = 16384
REACH = 7
KP = 8
X, Y, Z, M, H, S, R = range(7)
CM, CH, CS = 3, 4, 5


def partner(ids, e, k):
    return e + ids[e // 16, k, e % 16].astype(jnp.int32)


def direct(sides, dens_ref, acc_ref, tab, bc, wts, part, row_f, ids):
    for side, src in sides:
        h = src[64:80, :]
        s = -LOG2E / (h * h)
        for p in range(16):
            for c in range(5):
                tab[side * 16 + p, c, :] = src[c * 16 + p, :]
            tab[side * 16 + p, S, :] = s[p]

    def columns(e, slot, chans):
        t = tab[e].T
        for n, c in chans:
            bc[slot, n] = jnp.broadcast_to(t[:, c : c + 1], (128, 128))

    def spread(i, _):
        columns(9 + i, i, ((0, X), (1, Y), (2, Z), (3, S)))
        return 0

    lax.fori_loop(0, 30, spread, 0, unroll=2)

    def bcast(e, c):
        return tab[e, pl.ds(c, 8, stride=0), :][None]

    def dens_cell(i, store):
        e = 9 + i
        who = [e] + [partner(ids, e, k) for k in range(KP)]
        for g in range(4):
            rows = pl.ds(32 * g, 32)
            xi, yi, zi, si = [bc[i, n, rows, :].reshape(4, 8, 128) for n in range(4)]
            total = jnp.zeros((4, 8, 128), jnp.float32)
            for k, j in enumerate(who):
                dx = xi - bcast(j, X)
                dy = yi - bcast(j, Y)
                dz = zi - bcast(j, Z)
                w = jnp.exp2((dx * dx + dy * dy + dz * dz) * si) * bcast(j, M)
                total = total + w
                if store:
                    wts[i - 7, k, rows, :] = w.reshape(32, 128)
            part[i, rows, :] = total.reshape(32, 128)

    def own_dens(i, _):
        dens_cell(7 + i, True)
        return 0

    def rim_dens(i, _):
        dens_cell(jnp.where(i < 7, i, i + 16), False)
        return 0

    lax.fori_loop(0, 16, own_dens, 0)
    lax.fori_loop(0, 14, rim_dens, 0)
    ones = jnp.ones((8, 128), jnp.float32)

    def rowsum(v):
        return lax.dot_general(ones, v, (((1,), (1,)), ((), ())), precision=HI, preferred_element_type=jnp.float32)

    def finish(i, _):
        e = 9 + i
        t = rowsum(part[i])[0:1]
        h = tab[e, pl.ds(H, 1), :]
        live = tab[e, pl.ds(M, 1), :] > 0.0
        d = jnp.where(live, t / (h * h * h), 0.0)
        row_f[i] = jnp.broadcast_to(d, (8, 128))
        tab[e, pl.ds(R, 1), :] = jnp.where(live, 1.0 / jnp.where(live, d, 1.0), 0.0)
        return 0

    lax.fori_loop(0, 30, finish, 0, unroll=3)
    for p in range(16):
        dens_ref[p, :] = row_f[7 + p, 0]

    def spread_r(i, _):
        columns(16 + i, 7 + i, ((3, R),))
        return 0

    lax.fori_loop(0, 16, spread_r, 0, unroll=2)

    def force_cell(i, _):
        e = 16 + i
        who = [e] + [partner(ids, e, k) for k in range(KP)]
        for g in range(4):
            rows = pl.ds(32 * g, 32)
            xi, yi, zi, ri = [bc[7 + i, n, rows, :].reshape(4, 8, 128) for n in range(4)]
            fx = fy = fz = jnp.zeros((4, 8, 128), jnp.float32)
            for k, j in enumerate(who):
                c = wts[i, k, rows, :].reshape(4, 8, 128) * (ri + bcast(j, R))
                fx = fx + c * (xi - bcast(j, X))
                fy = fy + c * (yi - bcast(j, Y))
                fz = fz + c * (zi - bcast(j, Z))
            bc[7 + i, 0, rows, :] = fx.reshape(32, 128)
            bc[7 + i, 1, rows, :] = fy.reshape(32, 128)
            bc[7 + i, 2, rows, :] = fz.reshape(32, 128)
        return 0

    lax.fori_loop(0, 16, force_cell, 0)

    def finish_f(i, _):
        e = 16 + i
        s = tab[e, pl.ds(S, 1), :]
        live = tab[e, pl.ds(M, 1), :] > 0.0
        scale = jnp.where(live, s * (-2.0 / LOG2E), 0.0)
        for n in range(3):
            row_f[i, n] = (rowsum(bc[7 + i, n])[0:1] * scale)[0]
        return 0

    lax.fori_loop(0, 16, finish_f, 0, unroll=2)
    for p in range(16):
        for n in range(3):
            acc_ref[n, p, :] = row_f[p, n]


def split3(t):
    hi = t.astype(jnp.bfloat16).astype(jnp.float32)
    rest = t - hi
    mid = rest.astype(jnp.bfloat16).astype(jnp.float32)
    return hi, mid, (rest - mid).astype(jnp.bfloat16).astype(jnp.float32)


def expanded(dens_ref, acc_ref, com, tj, ti, left, right, rhs, whi, wlo, dsum, val, out, ids):
    bf16, f32 = jnp.bfloat16, jnp.float32
    lane = lax.broadcasted_iota(jnp.int32, (128, 128), 1)

    def columns(i, _):
        hi, mid, lo = split3(tj[2 + i])
        zero = jnp.zeros((8, 128), f32)
        half = [hi, mid, hi, lo, hi, mid, zero, zero]
        t = jnp.concatenate(half + half, 0).T
        left[2 + i] = jnp.where(lane < 64, t, 0.0).astype(bf16)
        right[2 + i] = jnp.where(lane < 64, 0.0, t).astype(bf16)
        return 0

    lax.fori_loop(0, 44, columns, 0, unroll=22)

    def rows(e):
        hi, mid, lo = split3(ti[e])
        zero = jnp.zeros((8, 128), f32)
        return jnp.concatenate([hi, hi, mid, hi, lo, mid, zero, zero], 0).astype(bf16)

    rim = [(0, 1), (2, 3), (4, 5), (6, 23), (24, 25), (26, 27), (28, 29)]
    blank = jnp.zeros((64, 128), bf16)
    for t, (i, j) in enumerate([(7 + 2 * t, 8 + 2 * t) for t in range(8)] + rim):
        rhs[t, 0:64, 0:128] = rows(9 + i)
        rhs[t, 0:64, 128:256] = blank
        rhs[t, 64:128, 0:128] = blank
        rhs[t, 64:128, 128:256] = rows(9 + j)

    def weights(t, i, j, store):
        a, b = 9 + i, 9 + j
        r = rhs[t]
        total = jnp.zeros((8, 256), f32)
        for k in range(KP + 1):
            p = a if k == 0 else partner(ids, a, k - 1)
            q = b if k == 0 else partner(ids, b, k - 1)
            e = jnp.dot(left[p] + right[q], r, preferred_element_type=f32)
            w = jnp.exp2(e)
            total = total + w.reshape(16, 8, 256).sum(0)
            if store:
                hi = w.astype(bf16)
                lo = (w - hi.astype(f32)).astype(bf16)
                at = pl.ds(128 * k, 128)
                whi[i - 7, at, :] = hi[:, :128]
                whi[j - 7, at, :] = hi[:, 128:]
                wlo[i - 7, at, :] = lo[:, :128]
                wlo[j - 7, at, :] = lo[:, 128:]
        dsum[i] = total[:, :128]
        dsum[j] = total[:, 128:]

    def own_pair(t, _):
        weights(t, 7 + 2 * t, 8 + 2 * t, True)
        return 0

    def rim_pair(t, _):
        i = jnp.where(t > 3, 16 + 2 * t, 2 * t)
        j = jnp.where(t > 2, 17 + 2 * t, 2 * t + 1)
        weights(8 + t, i, j, False)
        return 0

    lax.fori_loop(0, 8, own_pair, 0, unroll=8)
    lax.fori_loop(0, 7, rim_pair, 0, unroll=7)

    total = sum(dsum[:, n, :] for n in range(8))
    h = com[CH, 9:39, :]
    live = com[CM, 9:39, :] > 0.0
    dens = jnp.where(live, total / (h * h * h), 0.0)
    recip = jnp.where(live, 1.0 / jnp.where(live, dens, 1.0), 0.0)
    dens_ref[...] = dens[7:23]
    sub = lax.broadcasted_iota(jnp.int32, (8, 128), 0)
    zero = jnp.zeros((8, 128), f32)
    for i in range(30):
        t = tj[9 + i]
        v = jnp.where(sub < 4, t, pltpu.roll(t, 4, 0) * recip[i : i + 1])
        val[9 + i] = jnp.concatenate([*split3(v), zero], 0).astype(bf16)

    def force(i, _):
        e = 16 + i
        who = [e] + [partner(ids, e, k) for k in range(KP)]
        v = jnp.concatenate([val[j] for j in who], 1)
        o = jnp.dot(v, whi[i], preferred_element_type=f32) + jnp.dot(v, wlo[i], preferred_element_type=f32)
        out[i] = o[0:8] + o[8:16] + o[16:24]
        return 0

    lax.fori_loop(0, 16, force, 0, unroll=16)
    s = com[CS, 16:32, :]
    scale = jnp.where(live[7:23], s * (-2.0 / LOG2E), 0.0)
    r = recip[7:23]
    for n in range(3):
        u = com[n, 16:32, :]
        acc_ref[n] = scale * (r * (u * out[:, 0, :] - out[:, 1 + n, :]) + (u * out[:, 4, :] - out[:, 5 + n, :]))


def body(odd_of, own, mate, peer, dens_ref, acc_ref, com, tj, ti, left, right, rhs, whi, wlo, dsum, val, out,
         tab, bc, wts, part, row_f, ids, sems):
    odd = odd_of()
    sides = ((1, own), (2 - 2 * odd, mate), (2 * odd, peer))
    copies = []
    for n, (side, src) in enumerate(sides):
        copy = pltpu.make_async_copy(src.at[pl.ds(80, 8), :], ids.at[side], sems.at[n])
        copy.start()
        copies.append(copy)
    one = jnp.ones((1, 128), jnp.float32)
    centre = [jnp.broadcast_to(own[16 * c + 8 : 16 * c + 9, 0:1], (16, 128)) for c in range(3)]
    far = steep = jnp.zeros((16, 128), jnp.float32)
    for side, src in sides:
        u = [src[16 * c : 16 * c + 16, :] - centre[c] for c in range(3)]
        m = src[48:64, :]
        h = src[64:80, :]
        s = -LOG2E / (h * h)
        q = u[0] * u[0] + u[1] * u[1] + u[2] * u[2]
        lm = jnp.where(m > 0.0, jnp.log2(jnp.where(m > 0.0, m, 1.0)), -30000.0)
        far = jnp.maximum(far, q)
        steep = jnp.maximum(steep, -s)
        at = pl.ds(pl.multiple_of(side * 16, 16), 16)
        for c, x in enumerate((*u, m, h, s)):
            com[c, at, :] = x
        fi = (s * q, -2.0 * s * u[0], -2.0 * s * u[1], -2.0 * s * u[2], s)
        for p in range(16):
            e = side * 16 + p
            tj[e] = jnp.concatenate([one, *(x[p : p + 1] for x in (*u, q, lm)), 0.0 * one, 0.0 * one], 0)
            ti[e] = jnp.concatenate([*(x[p : p + 1] for x in fi), one, 0.0 * one, 0.0 * one], 0)
    near = jnp.max(far) * jnp.max(steep) < 2048.0
    for copy in copies:
        copy.wait()

    @pl.when(near)
    def _():
        expanded(dens_ref, acc_ref, com, tj, ti, left, right, rhs, whi, wlo, dsum, val, out, ids)

    @pl.when(jnp.logical_not(near))
    def _():
        direct(sides, dens_ref, acc_ref, tab, bc, wts, part, row_f, ids)


def call(own, mate, peer, odd_of):
    f32 = jnp.float32
    return pl.pallas_call(
        functools.partial(body, odd_of),
        out_shape=(jax.ShapeDtypeStruct((16, 128), f32), jax.ShapeDtypeStruct((3, 16, 128), f32)),
        in_specs=[pl.BlockSpec(memory_space=pltpu.VMEM)] * 3,
        out_specs=(pl.BlockSpec(memory_space=pltpu.VMEM),) * 2,
        scratch_shapes=[
            pltpu.VMEM((6, TABLE, 128), f32),
            pltpu.VMEM((TABLE, 8, 128), f32),
            pltpu.VMEM((TABLE, 8, 128), f32),
            pltpu.VMEM((TABLE, 128, 128), jnp.bfloat16),
            pltpu.VMEM((TABLE, 128, 128), jnp.bfloat16),
            pltpu.VMEM((15, 128, 256), jnp.bfloat16),
            pltpu.VMEM((16, 1152, 128), jnp.bfloat16),
            pltpu.VMEM((16, 1152, 128), jnp.bfloat16),
            pltpu.VMEM((30, 8, 128), f32),
            pltpu.VMEM((TABLE, 32, 128), jnp.bfloat16),
            pltpu.VMEM((16, 8, 128), f32),
            pltpu.VMEM((TABLE, 8, 128), f32),
            pltpu.VMEM((30, 4, 128, 128), f32),
            pltpu.VMEM((16, 9, 128, 128), f32),
            pltpu.VMEM((30, 128, 128), f32),
            pltpu.VMEM((30, 8, 128), f32),
            pltpu.SMEM((3, 8, 128), f32),
            pltpu.SemaphoreType.DMA((3,)),
        ],
        compiler_params=pltpu.CompilerParams(vmem_limit_bytes=40 << 20),
        name="sph",
    )(own, mate, peer)


def shards(position, mass, smooth, counts, partners):
    groups = lax.axis_size("group")
    devices = groups * lax.axis_size("curve")
    group = lax.axis_index("group")
    start = lax.axis_index("curve") * CURVE
    slots = position.shape[-1]
    alive = jnp.arange(slots, dtype=jnp.int32)[None, :] < counts[:, None]
    mlive = jnp.where(alive, mass, jnp.zeros_like(mass))
    step = partners.T - (start + jnp.arange(CURVE, dtype=jnp.int32))[None, :]
    step = jnp.where(step > REACH, step - NCELL, jnp.where(step < -REACH, step + NCELL, step))
    step = lax.dynamic_slice_in_dim(step.astype(jnp.float32), group * OWN, OWN, 1)
    step = jnp.pad(step, ((0, 0), (0, slots - OWN)))
    packed = jnp.concatenate([position.reshape(3 * OWN, slots), mlive, smooth, step], 0)
    axes = ("curve", "group")
    lap = 16 * groups
    edge = [(i, i ^ 1) for i in range(devices) if i % lap < 2]
    chip = [(i, i ^ 1) for i in range(devices) if i % lap >= 2]
    link = [(i, (i + 1 if i % 2 else i - 1) % devices) for i in range(devices)]
    first = lax.ppermute(packed, axes, edge)
    over_link = lax.ppermute(packed, axes, link)
    over_chip = first + lax.ppermute(packed, axes, chip)
    return call(packed, over_chip, over_link, lambda: lax.rem(lax.axis_index("group"), 2))


def solution(mesh):
    return jax.shard_map(
        shards,
        mesh=mesh,
        in_specs=(
            P(None, ("curve", "group"), None),
            P(("curve", "group"), None),
            P(("curve", "group"), None),
            P(("curve", "group")),
            P("curve", None),
        ),
        out_specs=(P(("curve", "group"), None), P(None, ("curve", "group"), None)),
        check_vma=False,
    )
```
